32 devices in a mesh: track: 16 (over z, y, x), cam: 2 (over core).
Axes of the slice: x: 2, y: 2, z: 4, core: 2. Of those that a mesh axis runs over, the one named last changes fastest.
Arguments:
- omega: bfloat16 [32, 9, 4096], P(None, None, ('track', 'cam')), may hold values from -6 to 6
- u_blocks: float32 [9, 9, 4096], P(None, None, ('track', 'cam')), may hold values from -5.4 to 36, as said below
- w_blocks: bfloat16 [9, 3, 16384], P(None, None, ('track', 'cam')), may hold values from -1.796875 to 1.796875
- v_inverse: float32 [3, 3, 4096], P(None, None, ('track', 'cam')), may hold values from -0.6 to 1.5, as said below
- obs_camera: int32 [16384], P(('track', 'cam')), may hold values from 0 to 4095, as said below
- obs_track: int32 [16384], P(('track', 'cam')), may hold values from 0 to 31, as said below
- obs_mask: int32 [16384], P(('track', 'cam')), may hold values from 0 to 1, as said below
Outputs:
- sketch: float32 [32, 9, 4096], P(None, None, ('track', 'cam'))
- basis: float32 [32, 9, 4096], P(None, None, ('track', 'cam'))
- factor: float32 [32, 32], replicated
The draws below stay inside these ranges and needn't reach their ends.
Inputs may be any that keep to these rules, and one draw needn't show every extreme that they name: `obs_camera`: cameras c * 128 to (c + 1) * 128 - 1 belong to device c (track slower). Among one device's 512 observations, padding included, at most 32 name cameras of any one device, and exactly 32 name those of some device. `obs_track`: in each aligned block of 128 observations, slots 0 to 31 each hold one track of 2 to 4 consecutive observations from the block's start, in rising order; the padding after them carries slot 31. `obs_mask`: 1 on the observations of tracks, 0 on the padding at the end of each block. `u_blocks`: each block is symmetric. `v_inverse`: each block is symmetric positive definite.
All inputs are finite; a program needn't handle non-finite values.
Results may differ from the reference program's by a relative error of at most 0.00095.
Values may be sent and summed in bfloat16 or wider, within the bound.
A program may use at most 64 MiB of HBM per device.

```python
import math
import jax
import jax.numpy as jnp
from jax import lax

CAM_PARAMS = 9
COLS = 32
BLK_OBS = 128
TRK_BLK = 32
CAM_DEV = 128
OBS_DEV = 512
CAMS = 4096
OBS = 16384
TRACKS = 4096


def track_layout(key):
    blocks = OBS // BLK_OBS
    lengths = jax.random.randint(key, (blocks, TRK_BLK), 2, 5)
    ends = jnp.cumsum(lengths, axis=1)
    position = jnp.arange(BLK_OBS, dtype=jnp.int32)
    slot_ids = jnp.sum((position[None, :, None] >= ends[:, None, :]).astype(jnp.int32), axis=2)
    live_ids = (slot_ids < TRK_BLK).astype(jnp.int32)
    slot_ids = jnp.minimum(slot_ids, TRK_BLK - 1)
    return (slot_ids.reshape(-1).astype(jnp.int32), live_ids.reshape(-1))


def draw_obs_track(key, part):
    return track_layout(jax.random.fold_in(key, 11))[0]


def draw_obs_mask(key, part):
    return track_layout(jax.random.fold_in(key, 11))[1]


def draw_obs_camera(key, part):
    device_count = OBS // OBS_DEV
    capacity = max(2, 2 * OBS_DEV // device_count)
    slot_total = device_count * capacity

    def one_device(device_key):
        keys = jax.random.split(device_key, 5)
        heat = jax.random.randint(keys[0], (device_count,), 0, 4)
        full_owner = jax.random.randint(keys[1], (), 0, device_count)
        owner_of = jnp.arange(slot_total, dtype=jnp.int32) // capacity
        score = jax.random.randint(keys[2], (slot_total,), 0, 65536) + heat[owner_of] * 16384
        score = jnp.where(owner_of == full_owner, score + 1048576, score)
        picked = jnp.argsort(-score, stable=True)[:OBS_DEV]
        cameras = owner_of[picked] * CAM_DEV + jax.random.randint(keys[3], (OBS_DEV,), 0, CAM_DEV)
        return cameras[jax.random.permutation(keys[4], OBS_DEV)]
    return jax.vmap(one_device)(jax.random.split(key, device_count)).reshape(-1).astype(jnp.int32)


def draw_u_blocks(key, part):
    keys = jax.random.split(key, 2)
    cam_index = jnp.arange(CAMS, dtype=jnp.float32)
    growth = 2.0
    scaling = 1.0 + growth * cam_index / (CAMS - 1)
    diagonal = jax.random.uniform(keys[0], (9, CAMS), jnp.float32, 2.0, 4.0)
    rough = jax.random.uniform(keys[1], (9, 9, CAMS), jnp.float32, -0.6, 0.6)
    symmetric = 0.5 * (rough + rough.transpose(1, 0, 2))
    identity = jnp.eye(9, dtype=jnp.float32)[:, :, None]
    blocks = symmetric * (1.0 - identity) + identity * diagonal[:, None, :]
    return (blocks * scaling[None, None, :]).astype(jnp.float32)


def draw_v_inverse(key, part):
    keys = jax.random.split(key, 2)
    low_end, high_end = (0.3, 1.0)
    diagonal = jnp.exp(jax.random.uniform(keys[0], (3, TRACKS), jnp.float32, math.log(low_end), math.log(high_end)))
    rough = jax.random.uniform(keys[1], (3, 3, TRACKS), jnp.float32, -1.0, 1.0)
    symmetric = 0.5 * (rough + rough.transpose(1, 0, 2))
    root_diag = jnp.sqrt(diagonal)
    coupling = 0.4 * symmetric * root_diag[:, None, :] * root_diag[None, :, :]
    identity = jnp.eye(3, dtype=jnp.float32)[:, :, None]
    return (coupling * (1.0 - identity) + identity * diagonal[:, None, :]).astype(jnp.float32)


def shard_levels(rng, shape, pieces, smallest, high):
    def one(axis_at, blocks):
        draws = jax.random.uniform(jax.random.fold_in(jax.random.fold_in(rng, 6), axis_at), (blocks,), jnp.float32, smallest / len(pieces), high / len(pieces))
        return jnp.repeat(jnp.exp(draws), shape[axis_at] // blocks).reshape((-1,) + (1,) * (len(shape) - axis_at - 1))

    loudness = one(*pieces[0])
    for cut in pieces[1:]:
        loudness = loudness * one(*cut)
    return loudness


def noise(rng, dims, width, most, shards=(), held_as=jnp.bfloat16):
    entries = jax.random.normal(rng, dims, jnp.float32) * width
    if len(shards) > 0:
        entries = shard_levels(rng, dims, shards, -0.22, 0.18) * entries
    return jnp.clip(entries, min=-most, max=most).astype(held_as)


def setup_inputs(seed: int = 0) -> dict:
    key_list = jax.random.split(jax.random.key(seed), 8)
    omega = noise(key_list[0], (COLS, CAM_PARAMS, CAMS), 1.0, 6.0, ((2, 32),))
    u_blocks = draw_u_blocks(jax.random.fold_in(key_list[7], 71), 0)
    w_blocks = noise(key_list[2], (CAM_PARAMS, 3, OBS), 0.3, 1.796875, ((2, 32),))
    v_inverse = draw_v_inverse(jax.random.fold_in(key_list[7], 71), 0)
    obs_camera = draw_obs_camera(jax.random.fold_in(key_list[7], 71), 0)
    obs_track = draw_obs_track(jax.random.fold_in(key_list[7], 71), 0)
    obs_mask = draw_obs_mask(jax.random.fold_in(key_list[7], 71), 0)
    return {"omega": omega, "u_blocks": u_blocks, "w_blocks": w_blocks, "v_inverse": v_inverse, "obs_camera": obs_camera, "obs_track": obs_track, "obs_mask": obs_mask}


HIGH = lax.Precision.HIGHEST

def eliminate(gathered, weight, inverse, slot_ids, live_ids):
    live_mask = live_ids.astype(jnp.float32)
    track_ids = jnp.arange(OBS_DEV, dtype=jnp.int32) // BLK_OBS * TRK_BLK + slot_ids
    weight_f = weight.astype(jnp.float32)
    projected = jnp.einsum('mio,mco->ico', weight_f, gathered.astype(jnp.float32), precision=HIGH) * live_mask
    track_sum = jax.ops.segment_sum(projected.transpose(2, 0, 1), track_ids, num_segments=OBS_DEV // BLK_OBS * TRK_BLK)
    solved = jnp.einsum('ijt,tjc->tic', inverse, track_sum, precision=HIGH)
    spread = solved[track_ids]
    returned = jnp.einsum('mio,oic->mco', weight_f, spread, precision=HIGH) * live_mask
    return returned.astype(jnp.bfloat16)

def reference(omega, u_blocks, w_blocks, v_inverse, obs_camera, obs_track, obs_mask):
    device_count = OBS // OBS_DEV
    tracks_dev = OBS_DEV // BLK_OBS * TRK_BLK
    weights = w_blocks.reshape(9, 3, device_count, OBS_DEV).transpose(2, 0, 1, 3)
    inverses = v_inverse.reshape(3, 3, device_count, tracks_dev).transpose(2, 0, 1, 3)
    cameras = obs_camera.reshape(device_count, OBS_DEV)
    slots = obs_track.reshape(device_count, OBS_DEV)
    masks = obs_mask.reshape(device_count, OBS_DEV)

    def visit_device(accumulated, device_part):
        weight, inverse, camera, slot_ids, live_ids = device_part
        gathered = jnp.take(omega, camera, axis=2).transpose(1, 0, 2)
        returned = eliminate(gathered, weight, inverse, slot_ids, live_ids)
        accumulated = accumulated.at[:, :, camera].add(returned.astype(jnp.float32).transpose(1, 0, 2))
        return (accumulated, None)
    accumulated, _ = lax.scan(visit_device, jnp.zeros(omega.shape, jnp.float32), (weights, inverses, cameras, slots, masks))
    own_term = jnp.einsum('mnk,jnk->jmk', u_blocks.astype(jnp.float32), omega.astype(jnp.float32), precision=HIGH)
    sketch = own_term - accumulated
    flat_rows = sketch.reshape(sketch.shape[0], -1)
    gram_matrix = jnp.dot(flat_rows.astype(jnp.float32), flat_rows.T.astype(jnp.float32), precision=HIGH, preferred_element_type=jnp.float32)
    lower_factor = jnp.linalg.cholesky(gram_matrix / flat_rows.shape[1])
    basis_rows = jax.scipy.linalg.solve_triangular(lower_factor, flat_rows, lower=True).reshape(sketch.shape)
    return (sketch, basis_rows, lower_factor.T)
```

```python
import functools

import jax
import jax.numpy as jnp
from jax import lax
from jax.experimental import pallas as pl
from jax.experimental.pallas import tpu as pltpu
from jax.sharding import PartitionSpec as P

BLK_OBS = 128
TRK_BLK = 32
LANES = 128
CHUNK = 1024

HIGH = lax.Precision.HIGHEST
MESH = pl.DeviceIdType.MESH
NT = (((1,), (1,)), ((), ()))
F32 = jnp.float32
BF16 = jnp.bfloat16


def dot(left, right, precision=None):
    return jnp.dot(left, right, precision=precision, preferred_element_type=F32)


def dot_nt(left, right, precision=None):
    return lax.dot_general(left, right, NT, precision=precision, preferred_element_type=F32)


def one_hot(condition):
    return jnp.where(condition, 1.0, 0.0).astype(BF16)


def rows_iota(shape):
    return lax.broadcasted_iota(jnp.int32, shape, 0)


def lanes_iota(shape):
    return lax.broadcasted_iota(jnp.int32, shape, 1)


def repeat(count, body):
    if count == 1:
        body(0)
    else:
        pl.loop(0, count)(body)


def kernel(
    sizes,
    omega_ref, u_ref, rows_ref, ints_ref, v_ref,
    sketch_ref, basis_ref, factor_ref,
    send1, recv1, send2, recv2, send3, recv3, gsend, grecv,
    to_track, from_track, wide, pick, own, incoming, sum_ref,
    send_sems, recv_sems,
):
    track_count, cam_count, params, columns, capacity, chunk = sizes
    devices = track_count * cam_count
    cam_width = omega_ref.shape[1]
    obs_count = rows_ref.shape[1]
    tracks = v_ref.shape[2]
    chunks = devices * capacity // chunk
    per_chunk = chunk // capacity
    me = lax.axis_index("track") * cam_count + lax.axis_index("cam")

    def peer(step):
        other = lax.rem(me + step, devices)
        return other, (other // cam_count, lax.rem(other, cam_count))

    barrier = pltpu.get_barrier_semaphore()

    @pl.loop(1, devices)
    def _(step):
        pl.semaphore_signal(barrier, inc=1, device_id=peer(step)[1], device_id_type=MESH)

    def scatter(index, src, dst):
        @pl.loop(1, devices)
        def _(step):
            other, where = peer(step)
            pltpu.make_async_remote_copy(
                src_ref=src.at[other],
                dst_ref=dst.at[me],
                send_sem=send_sems.at[index],
                recv_sem=recv_sems.at[index],
                device_id=where,
                device_id_type=MESH,
            ).start()

        pltpu.make_async_copy(src.at[me], dst.at[me], recv_sems.at[index]).start()

    def broadcast(index, src, dst):
        @pl.loop(1, devices)
        def _(step):
            pltpu.make_async_remote_copy(
                src_ref=src,
                dst_ref=dst.at[me],
                send_sem=send_sems.at[index],
                recv_sem=recv_sems.at[index],
                device_id=peer(step)[1],
                device_id_type=MESH,
            ).start()

        pltpu.make_async_copy(src, dst.at[me], recv_sems.at[index]).start()

    def arrive(index, dst):
        pltpu.make_async_copy(dst, dst, recv_sems.at[index]).wait()

    def sent(index, dst):
        part = dst.at[pl.ds(0, devices - 1)]
        pltpu.make_async_copy(part, part, send_sems.at[index]).wait()

    owner = ints_ref[0:1, :]
    track_id = ints_ref[1:2, :]
    owned = one_hot(rows_iota((devices, obs_count)) == owner)
    earlier = one_hot(rows_iota((obs_count, obs_count)) < lanes_iota((obs_count, obs_count)))
    ranks = dot(owned, earlier)
    rank = jnp.sum(ranks * owned.astype(F32), axis=0, keepdims=True).astype(jnp.int32)
    slot = owner * capacity + rank
    member = one_hot(rows_iota((tracks, obs_count)) == track_id)
    fields = rows_ref[...]
    fields = jnp.concatenate(
        [fields, jnp.zeros((LANES - fields.shape[0], obs_count), BF16)], axis=0
    )

    def place(part):
        slots = one_hot(rows_iota((chunk, obs_count)) + part * chunk == slot)
        send1[pl.ds(part * per_chunk, per_chunk)] = (
            dot_nt(slots, fields).astype(BF16).reshape(per_chunk, capacity, LANES)
        )
        to_track[part] = dot_nt(member, slots).astype(BF16)
        from_track[part] = dot_nt(slots, member).astype(BF16)

    repeat(chunks, place)

    pl.semaphore_wait(barrier, devices - 1)
    scatter(0, send1, recv1)

    for row in range(params):
        total = jnp.zeros((columns, cam_width), F32)
        for col in range(params):
            total += u_ref[row, col : col + 1, :] * omega_ref[
                col * columns : (col + 1) * columns, :
            ].astype(F32)
        own[row * columns : (row + 1) * columns, :] = total
    incoming[...] = jnp.zeros_like(incoming)

    eye = one_hot(rows_iota((LANES, LANES)) == lanes_iota((LANES, LANES)))
    field_count = rows_ref.shape[0]
    width = 3 * columns

    def project(part):
        block = recv1[pl.ds(part * per_chunk, per_chunk)].reshape(chunk, LANES)
        turned = dot_nt(eye[:field_count], block)
        wide[part] = turned
        number = turned[3 * params : 3 * params + 1] * 256.0 + turned[
            3 * params + 1 : 3 * params + 2
        ]
        chosen = one_hot(rows_iota((cam_width, chunk)) == number.astype(jnp.int32))
        pick[part] = chosen
        gathered = dot(omega_ref[...], chosen)
        pieces = []
        for comp in range(3):
            total = jnp.zeros((columns, chunk), F32)
            for row in range(params):
                at = comp * params + row
                total += turned[at : at + 1] * gathered[row * columns : (row + 1) * columns]
            pieces.append(total)
        if width < LANES:
            pieces.append(jnp.zeros((LANES - width, chunk), F32))
        projected = jnp.concatenate(pieces, axis=0)
        send2[pl.ds(part * per_chunk, per_chunk)] = (
            projected.T.astype(BF16).reshape(per_chunk, capacity, LANES)
        )

    arrive(0, recv1)
    repeat(chunks, project)
    scatter(1, send2, recv2)
    sum_ref[...] = jnp.zeros_like(sum_ref)

    def collect(part):
        block = recv2[pl.ds(part * per_chunk, per_chunk)].reshape(chunk, LANES)
        sum_ref[...] += dot(to_track[part], block)

    arrive(1, recv2)
    repeat(chunks, collect)
    summed = sum_ref[...].T
    pieces = []
    for row in range(3):
        total = jnp.zeros((columns, tracks), F32)
        for col in range(3):
            total += v_ref[row, col : col + 1, :] * summed[col * columns : (col + 1) * columns]
        pieces.append(total)
    if width < LANES:
        pieces.append(jnp.zeros((LANES - width, tracks), F32))
    solved = jnp.concatenate(pieces, axis=0).astype(BF16)

    def spread(part):
        send3[pl.ds(part * per_chunk, per_chunk)] = (
            dot_nt(from_track[part], solved).astype(BF16).reshape(per_chunk, capacity, LANES)
        )

    repeat(chunks, spread)
    scatter(2, send3, recv3)

    def gather_back(part):
        block = recv3[pl.ds(part * per_chunk, per_chunk)].reshape(chunk, LANES)
        turned = dot_nt(eye[:width], block)
        weights = wide[part]
        pieces = []
        for row in range(params):
            total = jnp.zeros((columns, chunk), F32)
            for comp in range(3):
                at = comp * params + row
                total += weights[at : at + 1] * turned[comp * columns : (comp + 1) * columns]
            pieces.append(total)
        contribution = jnp.concatenate(pieces, axis=0).astype(BF16)
        incoming[...] += dot_nt(contribution, pick[part])

    arrive(2, recv3)
    repeat(chunks, gather_back)

    sketch = own[...] - incoming[...]
    sketch_ref[...] = sketch
    flat = jnp.concatenate(
        [sketch[row * columns : (row + 1) * columns] for row in range(params)], axis=1
    )
    gram = dot_nt(flat, flat, HIGH)
    groups = LANES // columns
    tall = columns // groups
    gsend[...] = jnp.concatenate(
        [gram[part * tall : (part + 1) * tall] for part in range(groups)], axis=1
    )
    broadcast(3, gsend, grecv)
    arrive(3, grecv)
    packed = jnp.sum(grecv[...], axis=0)
    gram = jnp.concatenate(
        [packed[:, part * columns : (part + 1) * columns] for part in range(groups)], axis=0
    )
    work = jnp.concatenate(
        [
            gram / (params * cam_width * devices),
            jnp.where(
                rows_iota((columns, columns)) == lanes_iota((columns, columns)), 1.0, 0.0
            ),
        ],
        axis=1,
    )
    row_ids = rows_iota((columns, 1))
    for step in range(columns - 1):
        scale = work[:, step : step + 1] * (1.0 / work[step : step + 1, step : step + 1])
        work = work - jnp.where(row_ids > step, scale, 0.0) * work[step : step + 1]
    upper = work[:, :columns]
    on_diagonal = rows_iota((columns, columns)) == lanes_iota((columns, columns))
    on_upper = rows_iota((columns, columns)) <= lanes_iota((columns, columns))
    diagonal = jnp.sum(jnp.where(on_diagonal, upper, 0.0), axis=1, keepdims=True)
    root = 1.0 / jnp.sqrt(diagonal)
    factor_ref[...] = jnp.where(on_upper, upper * root, 0.0)
    inverse = work[:, columns:] * root
    basis = dot(inverse, flat, HIGH)
    for row in range(params):
        basis_ref[row * columns : (row + 1) * columns, :] = basis[
            :, row * cam_width : (row + 1) * cam_width
        ]

    sent(0, recv1)
    sent(1, recv2)
    sent(2, recv3)
    sent(3, grecv)


def on_device(omega, u_blocks, w_blocks, v_inverse, obs_camera, obs_track, obs_mask):
    track_count = lax.axis_size("track")
    cam_count = lax.axis_size("cam")
    devices = track_count * cam_count
    columns, params, cam_width = omega.shape
    obs_count = obs_camera.shape[0]
    tracks = v_inverse.shape[2]
    capacity = max(2, 2 * obs_count // devices)
    capacity = -(-capacity // 16) * 16
    slots = devices * capacity
    chunk = min(CHUNK, slots)
    chunks = slots // chunk

    table = omega.transpose(1, 0, 2).reshape(params * columns, cam_width)
    owner = obs_camera // cam_width
    local = obs_camera - owner * cam_width
    weights = w_blocks.transpose(1, 0, 2).reshape(3 * params, obs_count)
    weights = weights * obs_mask.astype(BF16)
    number = jnp.stack([local // 256, local % 256]).astype(BF16)
    fields = jnp.concatenate([weights, number], axis=0)
    fields = jnp.pad(fields, ((0, 32 - fields.shape[0]), (0, 0)))
    block = jnp.arange(obs_count, dtype=jnp.int32) // BLK_OBS
    ints = jnp.stack([owner, block * TRK_BLK + obs_track])

    sizes = (track_count, cam_count, params, columns, capacity, chunk)
    message = pltpu.VMEM((devices, capacity, LANES), BF16)
    tall = columns * columns // LANES
    sketch, basis, factor = pl.pallas_call(
        functools.partial(kernel, sizes),
        out_shape=(
            jax.ShapeDtypeStruct((params * columns, cam_width), F32),
            jax.ShapeDtypeStruct((params * columns, cam_width), F32),
            jax.ShapeDtypeStruct((columns, columns), F32),
        ),
        in_specs=[pl.BlockSpec(memory_space=pltpu.VMEM)] * 5,
        out_specs=(pl.BlockSpec(memory_space=pltpu.VMEM),) * 3,
        scratch_shapes=[message] * 6
        + [
            pltpu.VMEM((tall, LANES), F32),
            pltpu.VMEM((devices, tall, LANES), F32),
            pltpu.VMEM((chunks, tracks, chunk), BF16),
            pltpu.VMEM((chunks, chunk, tracks), BF16),
            pltpu.VMEM((chunks, 32, chunk), F32),
            pltpu.VMEM((chunks, cam_width, chunk), BF16),
            pltpu.VMEM((params * columns, cam_width), F32),
            pltpu.VMEM((params * columns, cam_width), F32),
            pltpu.VMEM((tracks, LANES), F32),
            pltpu.SemaphoreType.DMA((4,)),
            pltpu.SemaphoreType.DMA((4,)),
        ],
        compiler_params=pltpu.CompilerParams(collective_id=0, has_side_effects=True),
    )(table, u_blocks, fields, ints, v_inverse)

    def unfold(array):
        return array.reshape(params, columns, cam_width).transpose(1, 0, 2)

    return (unfold(sketch), unfold(basis), factor)


def solution(mesh):
    spread = P(None, None, ("track", "cam"))
    flat = P(("track", "cam"))
    return jax.shard_map(
        on_device,
        mesh=mesh,
        in_specs=(spread,) * 4 + (flat,) * 3,
        out_specs=(spread, spread, P()),
        check_vma=False,
    )
```

```python
import functools

import jax
import jax.numpy as jnp
from jax import lax
from jax.experimental import pallas as pl
from jax.experimental.pallas import tpu as pltpu
from jax.sharding import PartitionSpec as P

BLK_OBS = 128
TRK_BLK = 32
LANES = 128
CHUNK = 1024

HIGH = lax.Precision.HIGHEST
MESH = pl.DeviceIdType.MESH
NT = (((1,), (1,)), ((), ()))
F32 = jnp.float32
BF16 = jnp.bfloat16


def dot(left, right, precision=None):
    return jnp.dot(left, right, precision=precision, preferred_element_type=F32)


def dot_nt(left, right, precision=None):
    return lax.dot_general(left, right, NT, precision=precision, preferred_element_type=F32)


def one_hot(condition):
    return jnp.where(condition, 1.0, 0.0).astype(BF16)


def rows_iota(shape):
    return lax.broadcasted_iota(jnp.int32, shape, 0)


def lanes_iota(shape):
    return lax.broadcasted_iota(jnp.int32, shape, 1)


def repeat(count, body):
    if count == 1:
        body(0)
    else:
        pl.loop(0, count)(body)


def kernel(
    sizes,
    omega_ref, u_ref, w_ref, v_ref, camera_ref, track_ref, mask_ref,
    sketch_ref, basis_ref, factor_ref,
    send1, recv1, send2, recv2, send3, recv3, gsend, grecv,
    fields, to_track, wide, pick, own, incoming, sum_ref,
    send_sems, recv_sems,
):
    track_count, cam_count, params, columns, rows, groups, span = sizes
    devices = track_count * cam_count
    cam_width = omega_ref.shape[1]
    obs_count = camera_ref.shape[1]
    tracks = v_ref.shape[2]
    part_rows = span * rows
    chunk = groups * part_rows
    chunks = devices // span
    me = lax.axis_index("track") * cam_count + lax.axis_index("cam")

    def peer(turn):
        step = devices // 2 + (1 - 2 * lax.rem(turn, 2)) * ((turn + 1) // 2)
        other = lax.rem(me + step, devices)
        return other, (other // cam_count, lax.rem(other, cam_count))

    barrier = pltpu.get_barrier_semaphore()

    @pl.loop(0, devices - 1)
    def _(turn):
        pl.semaphore_signal(barrier, inc=1, device_id=peer(turn)[1], device_id_type=MESH)

    def scatter(index, src, dst):
        @pl.loop(0, devices - 1)
        def _(turn):
            other, where = peer(turn)
            pltpu.make_async_remote_copy(
                src_ref=src.at[other],
                dst_ref=dst.at[me],
                send_sem=send_sems.at[index],
                recv_sem=recv_sems.at[index],
                device_id=where,
                device_id_type=MESH,
            ).start()

        pltpu.make_async_copy(src.at[me], dst.at[me], recv_sems.at[index]).start()

    def broadcast(index, src, dst):
        @pl.loop(0, devices - 1)
        def _(turn):
            pltpu.make_async_remote_copy(
                src_ref=src,
                dst_ref=dst.at[me],
                send_sem=send_sems.at[index],
                recv_sem=recv_sems.at[index],
                device_id=peer(turn)[1],
                device_id_type=MESH,
            ).start()

        pltpu.make_async_copy(src, dst.at[me], recv_sems.at[index]).start()

    def arrive(index, dst):
        pltpu.make_async_copy(dst, dst, recv_sems.at[index]).wait()

    def sent(index, dst):
        part = dst.at[pl.ds(0, devices - 1)]
        pltpu.make_async_copy(part, part, send_sems.at[index]).wait()

    eye = one_hot(rows_iota((LANES, LANES)) == lanes_iota((LANES, LANES)))

    def pack(part, values, dst):
        for index in range(values.shape[0] // columns):
            block = values[index * columns : (index + 1) * columns]
            pieces = [block[:, g * part_rows : (g + 1) * part_rows] for g in range(groups)]
            if groups * columns < LANES:
                pieces.append(jnp.zeros((LANES - groups * columns, part_rows), F32))
            turned = jnp.concatenate(pieces, axis=0).T.reshape(span, rows, LANES)
            dst[pl.ds(part * span, span), index * rows : (index + 1) * rows] = turned.astype(BF16)

    def unpack(part, src):
        blocks = []
        for index in range(src.shape[1] // rows):
            block = src[pl.ds(part * span, span), index * rows : (index + 1) * rows]
            turned = dot_nt(eye, block.reshape(part_rows, LANES))
            blocks.append(
                jnp.concatenate(
                    [turned[g * columns : (g + 1) * columns] for g in range(groups)], axis=1
                )
            )
        return jnp.concatenate(blocks, axis=0)

    camera = camera_ref[...]
    owner = camera // cam_width
    local = camera - owner * cam_width
    track_id = lanes_iota((1, obs_count)) // BLK_OBS * TRK_BLK + track_ref[...]
    live = mask_ref[...].astype(F32)
    fields[...] = jnp.zeros_like(fields)
    for row in range(params):
        fields[3 * row : 3 * row + 3, :] = w_ref[row].astype(F32) * live
    high = local // 256
    fields[3 * params : 3 * params + 1, :] = high.astype(F32)
    fields[3 * params + 1 : 3 * params + 2, :] = (local - high * 256).astype(F32)
    owned = one_hot(rows_iota((devices, obs_count)) == owner)
    earlier = one_hot(rows_iota((obs_count, obs_count)) < lanes_iota((obs_count, obs_count)))
    ranks = dot(owned, earlier)
    rank = jnp.sum(ranks * owned.astype(F32), axis=0, keepdims=True).astype(jnp.int32)
    group = jnp.zeros_like(rank)
    for g in range(1, groups):
        group += jnp.where(rank >= g * rows, 1, 0)
    offset = group * part_rows + rank - group * rows
    member = one_hot(rows_iota((tracks, obs_count)) == track_id)
    table = jnp.concatenate([fields[...].astype(BF16), member], axis=0)

    def place(part):
        nearby = owner - part * span
        inside = jnp.logical_and(nearby >= 0, nearby < span)
        slot = jnp.where(inside, nearby * rows + offset, -1)
        slots = one_hot(rows_iota((chunk, obs_count)) == slot)
        placed = dot_nt(table, slots)
        pack(part, placed[:columns], send1)
        to_track[part] = placed[columns:].astype(BF16)

    repeat(chunks, place)

    pl.semaphore_wait(barrier, devices - 1)
    scatter(0, send1, recv1)

    for row in range(params):
        total = jnp.zeros((columns, cam_width), F32)
        for col in range(params):
            total += u_ref[row, col : col + 1, :] * omega_ref[
                col * columns : (col + 1) * columns, :
            ].astype(F32)
        own[row * columns : (row + 1) * columns, :] = total
    incoming[...] = jnp.zeros_like(incoming)
    sum_ref[...] = jnp.zeros_like(sum_ref)

    def project(part):
        turned = unpack(part, recv1)
        wide[part] = turned
        number = turned[3 * params : 3 * params + 1] * 256.0 + turned[
            3 * params + 1 : 3 * params + 2
        ]
        chosen = one_hot(rows_iota((cam_width, chunk)) == number.astype(jnp.int32))
        pick[part] = chosen
        gathered = dot(omega_ref[...], chosen)
        pieces = []
        for comp in range(3):
            total = jnp.zeros((columns, chunk), F32)
            for row in range(params):
                at = row * 3 + comp
                total += turned[at : at + 1] * gathered[row * columns : (row + 1) * columns]
            pieces.append(total)
        pack(part, jnp.concatenate(pieces, axis=0), send2)

    arrive(0, recv1)
    repeat(chunks, project)
    scatter(1, send2, recv2)

    def collect(part):
        sum_ref[...] += dot_nt(unpack(part, recv2).astype(BF16), to_track[part])

    arrive(1, recv2)
    repeat(chunks, collect)
    pieces = []
    for row in range(3):
        total = jnp.zeros((columns, tracks), F32)
        for col in range(3):
            total += v_ref[row, col : col + 1, :] * sum_ref[col * columns : (col + 1) * columns]
        pieces.append(total)
    solved = jnp.concatenate(pieces, axis=0).astype(BF16)

    def spread(part):
        pack(part, dot(solved, to_track[part]), send3)

    repeat(chunks, spread)
    scatter(2, send3, recv3)

    def gather_back(part):
        turned = unpack(part, recv3)
        weights = wide[part]
        pieces = []
        for row in range(params):
            total = jnp.zeros((columns, chunk), F32)
            for comp in range(3):
                at = row * 3 + comp
                total += weights[at : at + 1] * turned[comp * columns : (comp + 1) * columns]
            pieces.append(total)
        contribution = jnp.concatenate(pieces, axis=0).astype(BF16)
        incoming[...] += dot_nt(contribution, pick[part])

    arrive(2, recv3)
    repeat(chunks, gather_back)

    sketch = own[...] - incoming[...]
    sketch_ref[...] = sketch
    flat = jnp.concatenate(
        [sketch[row * columns : (row + 1) * columns] for row in range(params)], axis=1
    )
    gram = dot_nt(flat, flat, HIGH)
    folds = LANES // columns
    tall = columns // folds
    gsend[...] = jnp.concatenate(
        [gram[part * tall : (part + 1) * tall] for part in range(folds)], axis=1
    )
    broadcast(3, gsend, grecv)
    arrive(3, grecv)
    packed = jnp.sum(grecv[...], axis=0)
    gram = jnp.concatenate(
        [packed[:, part * columns : (part + 1) * columns] for part in range(folds)], axis=0
    )
    work = jnp.concatenate(
        [
            gram / (params * cam_width * devices),
            jnp.where(
                rows_iota((columns, columns)) == lanes_iota((columns, columns)), 1.0, 0.0
            ),
        ],
        axis=1,
    )
    row_ids = rows_iota((columns, 1))
    for step in range(columns - 1):
        scale = work[:, step : step + 1] * (1.0 / work[step : step + 1, step : step + 1])
        work = work - jnp.where(row_ids > step, scale, 0.0) * work[step : step + 1]
    upper = work[:, :columns]
    on_diagonal = rows_iota((columns, columns)) == lanes_iota((columns, columns))
    on_upper = rows_iota((columns, columns)) <= lanes_iota((columns, columns))
    diagonal = jnp.sum(jnp.where(on_diagonal, upper, 0.0), axis=1, keepdims=True)
    root = 1.0 / jnp.sqrt(diagonal)
    factor_ref[...] = jnp.where(on_upper, upper * root, 0.0)
    inverse = work[:, columns:] * root
    basis = dot(inverse, flat, HIGH)
    for row in range(params):
        basis_ref[row * columns : (row + 1) * columns, :] = basis[
            :, row * cam_width : (row + 1) * cam_width
        ]

    sent(0, recv1)
    sent(1, recv2)
    sent(2, recv3)
    sent(3, grecv)


def on_device(omega, u_blocks, w_blocks, v_inverse, obs_camera, obs_track, obs_mask):
    track_count = lax.axis_size("track")
    cam_count = lax.axis_size("cam")
    devices = track_count * cam_count
    columns, params, cam_width = omega.shape
    obs_count = obs_camera.shape[0]
    tracks = v_inverse.shape[2]
    capacity = max(2, 2 * obs_count // devices)
    rows = -(-capacity // (LANES // columns) // 8) * 8
    groups = -(-capacity // rows)
    span = devices
    while span * rows * groups > CHUNK and span % 2 == 0:
        span //= 2
    chunk = span * rows * groups
    chunks = devices // span

    table = omega.transpose(1, 0, 2).reshape(params * columns, cam_width)
    line = (1, obs_count)
    sizes = (track_count, cam_count, params, columns, rows, groups, span)
    small = pltpu.VMEM((devices, rows, LANES), BF16)
    message = pltpu.VMEM((devices, 3 * rows, LANES), BF16)
    tall = columns * columns // LANES
    sketch, basis, factor = pl.pallas_call(
        functools.partial(kernel, sizes),
        out_shape=(
            jax.ShapeDtypeStruct((params * columns, cam_width), F32),
            jax.ShapeDtypeStruct((params * columns, cam_width), F32),
            jax.ShapeDtypeStruct((columns, columns), F32),
        ),
        in_specs=[pl.BlockSpec(memory_space=pltpu.VMEM)] * 7,
        out_specs=(pl.BlockSpec(memory_space=pltpu.VMEM),) * 3,
        scratch_shapes=[small] * 2
        + [message] * 4
        + [
            pltpu.VMEM((tall, LANES), F32),
            pltpu.VMEM((devices, tall, LANES), F32),
            pltpu.VMEM((columns, obs_count), F32),
            pltpu.VMEM((chunks, tracks, chunk), BF16),
            pltpu.VMEM((chunks, columns, chunk), F32),
            pltpu.VMEM((chunks, cam_width, chunk), BF16),
            pltpu.VMEM((params * columns, cam_width), F32),
            pltpu.VMEM((params * columns, cam_width), F32),
            pltpu.VMEM((3 * columns, tracks), F32),
            pltpu.SemaphoreType.DMA((4,)),
            pltpu.SemaphoreType.DMA((4,)),
        ],
        compiler_params=pltpu.CompilerParams(collective_id=0, has_side_effects=True),
    )(
        table,
        u_blocks,
        w_blocks,
        v_inverse,
        obs_camera.reshape(line),
        obs_track.reshape(line),
        obs_mask.reshape(line),
    )

    def unfold(array):
        return array.reshape(params, columns, cam_width).transpose(1, 0, 2)

    return (unfold(sketch), unfold(basis), factor)


def solution(mesh):
    spread = P(None, None, ("track", "cam"))
    flat = P(("track", "cam"))
    return jax.shard_map(
        on_device,
        mesh=mesh,
        in_specs=(spread,) * 4 + (flat,) * 3,
        out_specs=(spread, spread, P()),
        check_vma=False,
    )
```

```python
import functools

import jax
import jax.numpy as jnp
from jax import lax
from jax.experimental import pallas as pl
from jax.experimental.pallas import tpu as pltpu
from jax.sharding import PartitionSpec as P

BLK_OBS = 128
TRK_BLK = 32
LANES = 128
CHUNK = 1024

HIGH = lax.Precision.HIGHEST
MESH = pl.DeviceIdType.MESH
NT = (((1,), (1,)), ((), ()))
F32 = jnp.float32
BF16 = jnp.bfloat16


def dot(left, right, precision=None):
    return jnp.dot(left, right, precision=precision, preferred_element_type=F32)


def dot_nt(left, right, precision=None):
    return lax.dot_general(left, right, NT, precision=precision, preferred_element_type=F32)


def one_hot(condition):
    return jnp.where(condition, 1.0, 0.0).astype(BF16)


def rows_iota(shape):
    return lax.broadcasted_iota(jnp.int32, shape, 0)


def lanes_iota(shape):
    return lax.broadcasted_iota(jnp.int32, shape, 1)


def repeat(count, body):
    if count == 1:
        body(0)
    else:
        pl.loop(0, count)(body)


def kernel(
    sizes,
    omega_hbm, u_hbm, w_hbm, v_hbm, camera_hbm, track_hbm, mask_hbm,
    sketch_ref, basis_ref, factor_ref,
    send1, recv1, send2, recv2, send3, recv3, gsend, grecv,
    fields, to_track, wide, pick, own, incoming, sum_ref,
    send_sems, recv_sems,
    omega_ref, u_ref, w_ref, v_ref, camera_ref, track_ref, mask_ref, load_sems,
):
    track_count, cam_count, params, columns, rows, groups, span = sizes
    devices = track_count * cam_count
    cam_width = omega_ref.shape[1]
    obs_count = camera_ref.shape[1]
    tracks = v_ref.shape[2]
    part_rows = span * rows
    chunk = groups * part_rows
    chunks = devices // span
    me = lax.axis_index("track") * cam_count + lax.axis_index("cam")

    def peer(turn):
        other = lax.rem(me + turn + 1, devices)
        return other, (other // cam_count, lax.rem(other, cam_count))

    barrier = pltpu.get_barrier_semaphore()

    @pl.loop(0, devices - 1)
    def _(turn):
        pl.semaphore_signal(barrier, inc=1, device_id=peer(turn)[1], device_id_type=MESH)

    loads = [
        pltpu.make_async_copy(source, target, load_sems.at[index])
        for index, (source, target) in enumerate(
            [
                (camera_hbm, camera_ref),
                (track_hbm, track_ref),
                (mask_hbm, mask_ref),
                (w_hbm, w_ref),
                (omega_hbm, omega_ref),
                (u_hbm, u_ref),
                (v_hbm, v_ref),
            ]
        )
    ]
    for load in loads:
        load.start()

    def scatter(index, src, dst):
        @pl.loop(0, devices - 1)
        def _(turn):
            other, where = peer(turn)
            pltpu.make_async_remote_copy(
                src_ref=src.at[other],
                dst_ref=dst.at[me],
                send_sem=send_sems.at[index],
                recv_sem=recv_sems.at[index],
                device_id=where,
                device_id_type=MESH,
            ).start()

        pltpu.make_async_copy(src.at[me], dst.at[me], recv_sems.at[index]).start()

    def broadcast(index, src, dst):
        @pl.loop(0, devices - 1)
        def _(turn):
            pltpu.make_async_remote_copy(
                src_ref=src,
                dst_ref=dst.at[me],
                send_sem=send_sems.at[index],
                recv_sem=recv_sems.at[index],
                device_id=peer(turn)[1],
                device_id_type=MESH,
            ).start()

        pltpu.make_async_copy(src, dst.at[me], recv_sems.at[index]).start()

    def arrive(index, dst):
        pltpu.make_async_copy(dst, dst, recv_sems.at[index]).wait()

    def sent(index, dst):
        part = dst.at[pl.ds(0, devices - 1)]
        pltpu.make_async_copy(part, part, send_sems.at[index]).wait()

    eye = one_hot(rows_iota((LANES, LANES)) == lanes_iota((LANES, LANES)))

    def pack(part, values, dst):
        for index in range(values.shape[0] // columns):
            block = values[index * columns : (index + 1) * columns]
            pieces = [block[:, g * part_rows : (g + 1) * part_rows] for g in range(groups)]
            if groups * columns < LANES:
                pieces.append(jnp.zeros((LANES - groups * columns, part_rows), F32))
            turned = jnp.concatenate(pieces, axis=0).T.reshape(span, rows, LANES)
            dst[pl.ds(part * span, span), index * rows : (index + 1) * rows] = turned.astype(BF16)

    def unpack(part, src):
        blocks = []
        for index in range(src.shape[1] // rows):
            block = src[pl.ds(part * span, span), index * rows : (index + 1) * rows]
            turned = dot_nt(eye, block.reshape(part_rows, LANES))
            blocks.append(
                jnp.concatenate(
                    [turned[g * columns : (g + 1) * columns] for g in range(groups)], axis=1
                )
            )
        return jnp.concatenate(blocks, axis=0)

    for load in loads[:4]:
        load.wait()
    camera = camera_ref[...]
    owner = camera // cam_width
    local = camera - owner * cam_width
    track_id = lanes_iota((1, obs_count)) // BLK_OBS * TRK_BLK + track_ref[...]
    live = mask_ref[...].astype(F32)
    fields[...] = jnp.zeros_like(fields)
    for row in range(params):
        fields[3 * row : 3 * row + 3, :] = w_ref[row].astype(F32) * live
    high = local // 256
    fields[3 * params : 3 * params + 1, :] = high.astype(F32)
    fields[3 * params + 1 : 3 * params + 2, :] = (local - high * 256).astype(F32)
    owned = one_hot(rows_iota((devices, obs_count)) == owner)
    earlier = one_hot(rows_iota((obs_count, obs_count)) < lanes_iota((obs_count, obs_count)))
    ranks = dot(owned, earlier)
    rank = jnp.sum(ranks * owned.astype(F32), axis=0, keepdims=True).astype(jnp.int32)
    group = jnp.zeros_like(rank)
    for g in range(1, groups):
        group += jnp.where(rank >= g * rows, 1, 0)
    offset = group * part_rows + rank - group * rows
    member = one_hot(rows_iota((tracks, obs_count)) == track_id)
    table = jnp.concatenate([fields[...].astype(BF16), member], axis=0)

    def place(part):
        nearby = owner - part * span
        inside = jnp.logical_and(nearby >= 0, nearby < span)
        slot = jnp.where(inside, nearby * rows + offset, -1)
        slots = one_hot(rows_iota((chunk, obs_count)) == slot)
        placed = dot_nt(table, slots)
        pack(part, placed[:columns], send1)
        to_track[part] = placed[columns:].astype(BF16)

    repeat(chunks, place)

    pl.semaphore_wait(barrier, devices - 1)
    scatter(0, send1, recv1)

    for load in loads[4:]:
        load.wait()
    for row in range(params):
        total = jnp.zeros((columns, cam_width), F32)
        for col in range(params):
            total += u_ref[row, col : col + 1, :] * omega_ref[
                col * columns : (col + 1) * columns, :
            ].astype(F32)
        own[row * columns : (row + 1) * columns, :] = total
    incoming[...] = jnp.zeros_like(incoming)
    sum_ref[...] = jnp.zeros_like(sum_ref)

    def project(part):
        turned = unpack(part, recv1)
        wide[part] = turned
        number = turned[3 * params : 3 * params + 1] * 256.0 + turned[
            3 * params + 1 : 3 * params + 2
        ]
        chosen = one_hot(rows_iota((cam_width, chunk)) == number.astype(jnp.int32))
        pick[part] = chosen
        gathered = dot(omega_ref[...], chosen)
        pieces = []
        for comp in range(3):
            total = jnp.zeros((columns, chunk), F32)
            for row in range(params):
                at = row * 3 + comp
                total += turned[at : at + 1] * gathered[row * columns : (row + 1) * columns]
            pieces.append(total)
        pack(part, jnp.concatenate(pieces, axis=0), send2)

    arrive(0, recv1)
    repeat(chunks, project)
    scatter(1, send2, recv2)

    def collect(part):
        sum_ref[...] += dot_nt(unpack(part, recv2).astype(BF16), to_track[part])

    arrive(1, recv2)
    repeat(chunks, collect)
    pieces = []
    for row in range(3):
        total = jnp.zeros((columns, tracks), F32)
        for col in range(3):
            total += v_ref[row, col : col + 1, :] * sum_ref[col * columns : (col + 1) * columns]
        pieces.append(total)
    solved = jnp.concatenate(pieces, axis=0).astype(BF16)

    def spread(part):
        pack(part, dot(solved, to_track[part]), send3)

    repeat(chunks, spread)
    scatter(2, send3, recv3)

    def gather_back(part):
        turned = unpack(part, recv3)
        weights = wide[part]
        pieces = []
        for row in range(params):
            total = jnp.zeros((columns, chunk), F32)
            for comp in range(3):
                at = row * 3 + comp
                total += weights[at : at + 1] * turned[comp * columns : (comp + 1) * columns]
            pieces.append(total)
        contribution = jnp.concatenate(pieces, axis=0).astype(BF16)
        incoming[...] += dot_nt(contribution, pick[part])

    arrive(2, recv3)
    repeat(chunks, gather_back)

    sketch = own[...] - incoming[...]
    sketch_ref[...] = sketch
    flat = jnp.concatenate(
        [sketch[row * columns : (row + 1) * columns] for row in range(params)], axis=1
    )
    gram = dot_nt(flat, flat, HIGH)
    folds = LANES // columns
    tall = columns // folds
    gsend[...] = jnp.concatenate(
        [gram[part * tall : (part + 1) * tall] for part in range(folds)], axis=1
    )
    broadcast(3, gsend, grecv)
    arrive(3, grecv)
    packed = jnp.sum(grecv[...], axis=0)
    gram = jnp.concatenate(
        [packed[:, part * columns : (part + 1) * columns] for part in range(folds)], axis=0
    )
    work = jnp.concatenate(
        [
            gram / (params * cam_width * devices),
            jnp.where(
                rows_iota((columns, columns)) == lanes_iota((columns, columns)), 1.0, 0.0
            ),
        ],
        axis=1,
    )
    row_ids = rows_iota((columns, 1))
    for step in range(columns - 1):
        scale = work[:, step : step + 1] * (1.0 / work[step : step + 1, step : step + 1])
        work = work - jnp.where(row_ids > step, scale, 0.0) * work[step : step + 1]
    upper = work[:, :columns]
    on_diagonal = rows_iota((columns, columns)) == lanes_iota((columns, columns))
    on_upper = rows_iota((columns, columns)) <= lanes_iota((columns, columns))
    diagonal = jnp.sum(jnp.where(on_diagonal, upper, 0.0), axis=1, keepdims=True)
    root = 1.0 / jnp.sqrt(diagonal)
    factor_ref[...] = jnp.where(on_upper, upper * root, 0.0)
    inverse = work[:, columns:] * root
    basis = dot(inverse, flat, HIGH)
    for row in range(params):
        basis_ref[row * columns : (row + 1) * columns, :] = basis[
            :, row * cam_width : (row + 1) * cam_width
        ]

    sent(0, recv1)
    sent(1, recv2)
    sent(2, recv3)
    sent(3, grecv)


def on_device(omega, u_blocks, w_blocks, v_inverse, obs_camera, obs_track, obs_mask):
    track_count = lax.axis_size("track")
    cam_count = lax.axis_size("cam")
    devices = track_count * cam_count
    columns, params, cam_width = omega.shape
    obs_count = obs_camera.shape[0]
    tracks = v_inverse.shape[2]
    capacity = max(2, 2 * obs_count // devices)
    rows = -(-capacity // (LANES // columns) // 8) * 8
    groups = -(-capacity // rows)
    span = devices
    while span * rows * groups > CHUNK and span % 2 == 0:
        span //= 2
    chunk = span * rows * groups
    chunks = devices // span

    table = omega.transpose(1, 0, 2).reshape(params * columns, cam_width)
    line = (1, obs_count)
    operands = (
        table,
        u_blocks,
        w_blocks,
        v_inverse,
        obs_camera.reshape(line),
        obs_track.reshape(line),
        obs_mask.reshape(line),
    )
    sizes = (track_count, cam_count, params, columns, rows, groups, span)
    small = pltpu.VMEM((devices, rows, LANES), BF16)
    message = pltpu.VMEM((devices, 3 * rows, LANES), BF16)
    tall = columns * columns // LANES
    sketch, basis, factor = pl.pallas_call(
        functools.partial(kernel, sizes),
        out_shape=(
            pltpu.VMEM((params * columns, cam_width), F32),
            pltpu.VMEM((params * columns, cam_width), F32),
            pltpu.VMEM((columns, columns), F32),
        ),
        in_specs=[pl.BlockSpec(memory_space=pl.ANY)] * 7,
        out_specs=(pl.BlockSpec(memory_space=pltpu.VMEM),) * 3,
        scratch_shapes=[small] * 2
        + [message] * 4
        + [
            pltpu.VMEM((tall, LANES), F32),
            pltpu.VMEM((devices, tall, LANES), F32),
            pltpu.VMEM((columns, obs_count), F32),
            pltpu.VMEM((chunks, tracks, chunk), BF16),
            pltpu.VMEM((chunks, columns, chunk), F32),
            pltpu.VMEM((chunks, cam_width, chunk), BF16),
            pltpu.VMEM((params * columns, cam_width), F32),
            pltpu.VMEM((params * columns, cam_width), F32),
            pltpu.VMEM((3 * columns, tracks), F32),
            pltpu.SemaphoreType.DMA((4,)),
            pltpu.SemaphoreType.DMA((4,)),
        ]
        + [pltpu.VMEM(array.shape, array.dtype) for array in operands]
        + [pltpu.SemaphoreType.DMA((len(operands),))],
        compiler_params=pltpu.CompilerParams(collective_id=0, has_side_effects=True),
    )(*operands)

    def unfold(array):
        return array.reshape(params, columns, cam_width).transpose(1, 0, 2)

    return (unfold(sketch), unfold(basis), factor)


def solution(mesh):
    spread = P(None, None, ("track", "cam"))
    flat = P(("track", "cam"))
    return jax.shard_map(
        on_device,
        mesh=mesh,
        in_specs=(spread,) * 4 + (flat,) * 3,
        out_specs=(spread, spread, P()),
        check_vma=False,
    )
```
